32 devices in a mesh: dp: 2 (over x), vocab: 16 (over z, y, core).
Axes of the slice: x: 2, y: 2, z: 4, core: 2. Of those that a mesh axis runs over, the one named last changes fastest.
Arguments:
- hidden: bfloat16 [96, 8192], P('dp', 'vocab'), may hold values from -90 to 90
- weight: bfloat16 [8192, 38016], P('dp', 'vocab'), may hold values from -0.1875 to 0.1875
- targets: int32 [96], P('dp'), may hold values from 0 to 38015
- pad_mask: int32 [96], P('dp'), may hold values from 0 to 1
Outputs:
- token_nll: float32 [96], P('dp')
- nll_total: float32 [], replicated
The draws below stay inside these ranges and needn't reach their ends.
All inputs are finite; a program needn't handle non-finite values.
Results may differ from the reference program's by a relative error of at most 0.0003.
Values may be sent and summed in bfloat16 or wider, within the bound.
No kernel may reach another device: no remote copies, remote signals or barrier semaphores. Data moves between devices by JAX's collectives and lax.ppermute only.
A program may use at most 64 MiB of HBM per device.

```python
import math
import jax
import jax.numpy as jnp
import numpy as np

D = 8192
TOKENS = 96
VOCAB = 38016
N_DP = 2


def draw_hidden(key, part):
    base = jax.random.truncated_normal(key, -6.0, 6.0, (TOKENS, D), jnp.float32)
    return base.astype(jnp.bfloat16)


def draw_pad_mask(key, part):
    positions = jnp.arange(TOKENS)
    level = 25 + 70 * positions // TOKENS
    return (jax.random.randint(key, (TOKENS,), 0, 100) < level).astype(jnp.int32)


def set_ends(values, own_key, least, largest):
    shape = values.shape
    place = [jax.random.randint(jax.random.fold_in(own_key, axis), (), 0, shape[axis]) for axis in range(len(shape))]
    values = values.at[tuple(place)].set(least)
    longest = shape.index(max(shape))
    place[longest] = (place[longest] + 1) % shape[longest]
    return values.at[tuple(place)].set(largest)


def level_of(rng, dims, shards, low, high):
    factor_of, own = 1.0, jax.random.fold_in(rng, 6)
    for dim, shards_of in shards:
        heights = jnp.exp(jax.random.uniform(jax.random.fold_in(own, dim), (shards_of,), jnp.float32, low / len(shards), high / len(shards)))
        factor_of = factor_of * jnp.repeat(heights, dims[dim] // shards_of).reshape([-1 if axis == dim else 1 for axis in range(len(dims))])
    return factor_of


def rank_bounds(amount, skew):
    portions = [(1 << 20) // math.isqrt(rank ** skew) + 1 for rank in range(1, amount + 1)]
    deviation = 1 + sum(portions) // (1 << 30)
    return np.cumsum(np.array([max(1, weight // deviation) for weight in portions]))


def ranked_ids(stream_key, extent, number_of, skew):
    grid = rank_bounds(number_of, skew)
    ticket = jax.random.randint(jax.random.fold_in(stream_key, 1), extent, 0, int(grid[number_of - 1]))
    grade = jnp.searchsorted(jnp.asarray(grid, jnp.int32), ticket, side="right")
    return jax.random.permutation(jax.random.fold_in(stream_key, 2), number_of)[grade].astype(jnp.int32)


def normal_values(own_key, dims, spread, limit, pieces=(), held_as=jnp.bfloat16):
    entries = jax.random.normal(own_key, dims, jnp.float32) * spread
    if len(pieces) > 0:
        entries = level_of(own_key, dims, pieces, -0.22, 0.18) * entries
    return jnp.clip(entries, min=-limit, max=limit).astype(held_as)


def setup_inputs(seed: int = 0) -> dict:
    keys = jax.random.split(jax.random.key(seed), 5)
    hidden = draw_hidden(jax.random.fold_in(keys[4], 71), 0)
    weight = normal_values(keys[1], (D, VOCAB), (D // 9) ** -0.5, 0.1875, ((0, 2), (1, 16)))
    targets = set_ends(ranked_ids(keys[2], (TOKENS,), VOCAB, 2), jax.random.fold_in(keys[2], 3), 0, VOCAB - 1).astype(jnp.int32)
    pad_mask = draw_pad_mask(jax.random.fold_in(keys[4], 71), 0)
    return {"hidden": hidden, "weight": weight, "targets": targets, "pad_mask": pad_mask}


def reference(hidden, weight, targets, pad_mask):
    slab = D // N_DP
    logits = jnp.zeros((TOKENS, VOCAB), jnp.float32)
    for block in range(N_DP):
        partial_value = jnp.dot(hidden[:, block * slab:(block + 1) * slab], weight[block * slab:(block + 1) * slab, :], preferred_element_type=jnp.float32)
        logits = logits + partial_value
    row_max = jnp.max(logits, axis=1)
    exp_sum = jnp.sum(jnp.exp(logits - row_max[:, None]), axis=1)
    picked = jnp.take_along_axis(logits, targets[:, None].astype(jnp.int32), axis=1)[:, 0]
    token_nll = pad_mask.astype(jnp.float32) * (row_max + jnp.log(exp_sum) - picked)
    return token_nll, jnp.sum(token_nll)
```

```python
import jax
import jax.numpy as jnp
from jax import lax
from jax.experimental import pallas as pl
from jax.experimental.pallas import tpu as pltpu
from jax.sharding import PartitionSpec as P

AXES = ("dp", "vocab")


def move(value, sizes, route):
    dp_size, vocab_size = sizes
    pairs = []
    for d in range(dp_size):
        for v in range(vocab_size):
            to_d, to_v = route(d, v)
            pairs.append((d * vocab_size + v, to_d * vocab_size + to_v))
    return lax.ppermute(value, AXES, pairs)


def swap(value, sizes, bits):
    return move(value, sizes, lambda d, v: (d, v ^ bits))


def dot_kernel(first_col, place_ref, pieces_ref, weight_ref, out_ref):
    n_slices, n_tok, width = pieces_ref.shape
    n_cols = out_ref.shape[1]
    own = place_ref[0]
    total = jnp.zeros((n_cols, n_tok), jnp.float32)
    for index in range(n_slices):
        total += lax.dot_general(
            weight_ref[pl.ds(first_col, n_cols), pl.ds(index * width, width)],
            pieces_ref[index ^ own],
            (((1,), (1,)), ((), ())),
            preferred_element_type=jnp.float32,
        )
    out_ref[...] = total.T


def partial_logits(place, pieces, columns, first_col, n_cols):
    n_slices, n_tok, width = pieces.shape
    return pl.pallas_call(
        lambda *refs: dot_kernel(first_col, *refs),
        out_shape=jax.ShapeDtypeStruct((n_tok, n_cols), jnp.float32),
        in_specs=[pl.BlockSpec(memory_space=pltpu.SMEM)]
        + [pl.BlockSpec(memory_space=pltpu.VMEM)] * 2,
        out_specs=pl.BlockSpec(memory_space=pltpu.VMEM),
        compiler_params=pltpu.CompilerParams(vmem_limit_bytes=14 << 20),
        cost_estimate=pl.CostEstimate(
            flops=2 * n_slices * n_tok * width * n_cols * 3, bytes_accessed=0, transcendentals=0
        ),
    )(place, pieces, columns)


def join(parts):
    top = parts[0][0]
    for part in parts[1:]:
        top = jnp.maximum(top, part[0])
    total = sum(part[1] * jnp.exp(part[0] - top) for part in parts)
    return jnp.stack([top, total, sum(part[2] for part in parts)])


def per_device(hidden, weight, targets, pad_mask):
    sizes = dp_size, vocab_size = lax.axis_size("dp"), lax.axis_size("vocab")
    n_slices = vocab_size // dp_size
    tok, width = hidden.shape
    rows, n_cols = weight.shape
    d, v = lax.axis_index("dp"), lax.axis_index("vocab")

    columns = weight.T

    moved = [
        move(hidden, sizes, lambda a, b, o=o: (b // n_slices, (a + o) % dp_size * n_slices + b % n_slices))
        for o in range(dp_size)
    ]
    mine = v // n_slices
    pieces = jnp.concatenate(
        [lax.select_n((mine - t) % dp_size, *moved) if dp_size > 2
         else jnp.where(mine == t, moved[0], moved[1]) for t in range(dp_size)], axis=0
    )[None]
    bits = []
    bit = 1
    while bit < n_slices:
        bits.append(bit)
        bit *= 2
    order = bits[1:] + bits[:1]
    if len(order) > 2:
        one, two = order[0], order[1]
        base = pieces
        pieces_of = {0: base}
        for flip in (one, two, one | two):
            pieces_of[flip] = swap(base, sizes, flip)
        done, rest = [0, one, two, one | two], order[2:]
    else:
        pieces_of, done, rest = {0: pieces}, [0], order
    stack = jnp.concatenate([pieces_of[e] for e in done], axis=0)
    for flip in rest:
        stack = jnp.concatenate([stack, swap(stack, sizes, flip)], axis=0)
        done = done + [e ^ flip for e in done]
    place_of = [done.index(e) for e in range(n_slices)]
    if place_of != list(range(n_slices)):
        stack = jnp.stack([stack[i] for i in place_of])

    place = (v % n_slices).astype(jnp.int32)[None]
    cut = (n_cols // 2 + 127) // 128 * 128
    spans = [(0, cut), (cut, n_cols - cut)]
    col_ids = lax.broadcasted_iota(jnp.int32, (1, n_cols), 1) + v * n_cols
    sums = []
    for first, count in spans:
        part = partial_logits(place, stack, columns, first, count)
        part = part.reshape(dp_size, tok, count)
        kept = lax.dynamic_index_in_dim(part, d, 0, False)
        for o in range(1, dp_size):
            sent = lax.dynamic_index_in_dim(part, (d + o) % dp_size, 0, False)
            kept = kept + move(sent, sizes, lambda a, b, o=o: ((a + o) % dp_size, b))
        sums.append(kept)

    tops = [jnp.max(s, axis=1) for s in sums]
    found = []
    for (first, count), top, part in zip(spans, tops, sums):
        hit = col_ids[:, first:first + count] == targets[:, None]
        found.append(jnp.stack([
            top,
            jnp.sum(jnp.exp(part - top[:, None]), axis=1),
            jnp.sum(jnp.where(hit, part, 0.0), axis=1),
        ]))
    stats = join(found)
    bit = 1
    while bit < vocab_size:
        stats = join([stats, swap(stats, sizes, bit)])
        bit *= 2
    token_nll = pad_mask.astype(jnp.float32) * (stats[0] + jnp.log(stats[1]) - stats[2])
    total = jnp.sum(token_nll)[None]
    others = [total] + [
        move(total, sizes, lambda a, b, o=o: ((a + o) % dp_size, b)) for o in range(1, dp_size)
    ]
    ranked = [lax.select_n((d - t) % dp_size, *others) if dp_size > 2
              else jnp.where(d == t, others[0], others[1]) for t in range(dp_size)]
    return token_nll, sum(ranked)[0]


def solution(mesh):
    placed = (P("dp", "vocab"), P("dp", "vocab"), P("dp"), P("dp"))
    return jax.shard_map(
        per_device, mesh=mesh, in_specs=placed, out_specs=(P("dp"), P()), check_vma=False
    )
```
